32 devices in a mesh: dp: 4 (over x, y), tp: 8 (over z, core).
Axes of the slice: x: 2, y: 2, z: 4, core: 2. Of those that a mesh axis runs over, the one named last changes fastest.
Arguments:
- x: bfloat16 [4096, 12288], P(('dp', 'tp')), parts along dimension 0
- gain: bfloat16 [12288], replicated
- wq: bfloat16 [12288, 12288], P(None, 'tp')
- wk: bfloat16 [12288, 1024], P(None, 'tp')
- wv: bfloat16 [12288, 1024], P(None, 'tp')
- wo: bfloat16 [12288, 12288], P('tp')
Outputs:
- output: bfloat16 [4096, 12288], P(('dp', 'tp')), parts along dimension 0
There are 4 independent parts. The reference program is written for one: setup_inputs(seed, part) draws one part's arguments, and reference() takes and returns one part's arrays. A program takes and returns all parts, laid end to end along the dimension named above; an argument that names none is the same for every part.
All inputs are finite; a program needn't handle non-finite values.
Results may differ from the reference program's by a relative error of at most 0.012.
Values are sent between devices in bfloat16 or wider.
A program may use at most 2 GiB of HBM per device.

```python
import jax
import jax.numpy as jnp
from jax import lax

ROWS = 1024
D = 12288
HEADS = 96
KV_HEADS = 8
HEAD = 128
THETA = 10000


def setup_inputs(seed: int = 0, part: int = 0) -> dict:
    kx, kn, kq, kk, kv, ko = jax.random.split(jax.random.key(seed), 6)

    def weights(key, rows, columns):
        return jax.random.normal(key, (rows, columns), jnp.float32) * rows**-0.5

    drawn = {
        "x": jax.random.normal(jax.random.fold_in(kx, part), (ROWS, D), jnp.float32),
        "gain": 1 + 0.1 * jax.random.normal(kn, (D,), jnp.float32),
        "wq": 2 * weights(kq, D, HEADS * HEAD),
        "wk": 2 * weights(kk, D, KV_HEADS * HEAD),
        "wv": 4 * weights(kv, D, KV_HEADS * HEAD),
        "wo": weights(ko, HEADS * HEAD, D),
    }
    return {k: v.astype(jnp.bfloat16) for k, v in drawn.items()}


def normed(x, gain):
    wide = x.astype(jnp.float32)
    scale = lax.rsqrt(jnp.mean(wide * wide, -1, keepdims=True) + 1e-6)
    return (wide * scale * gain.astype(jnp.float32)).astype(jnp.bfloat16)


def turned(t, place, theta):
    half = t.shape[-1] // 2
    angle = place.astype(jnp.float32)[:, None] * theta ** (-jnp.arange(half, dtype=jnp.float32) / half)
    cos, sin = jnp.cos(angle)[:, None], jnp.sin(angle)[:, None]
    a, b = t[..., :half].astype(jnp.float32), t[..., half:].astype(jnp.float32)
    return jnp.concatenate([a * cos - b * sin, b * cos + a * sin], -1).astype(jnp.bfloat16)


def matmul(a, w):
    return jnp.dot(a, w, preferred_element_type=jnp.float32).astype(jnp.bfloat16)


def einsum(form, a, b):
    return jnp.einsum(form, a.astype(jnp.float32), b.astype(jnp.float32))


def attention(q, k, v):
    scores = einsum("tgsd,ugd->gstu", q, k) * q.shape[-1] ** -0.5
    token = jnp.arange(q.shape[0])
    scores = jnp.where(token[:, None] >= token, scores, -jnp.inf)
    weights = jax.nn.softmax(scores, -1).astype(jnp.bfloat16)
    return einsum("gstu,ugd->tgsd", weights, v).astype(jnp.bfloat16)


def reference(x, gain, wq, wk, wv, wo):
    a, place = normed(x, gain), jnp.arange(ROWS)
    q = turned(matmul(a, wq).reshape(ROWS, HEADS, HEAD), place, THETA).reshape(ROWS, KV_HEADS, -1, HEAD)
    k = turned(matmul(a, wk).reshape(ROWS, KV_HEADS, HEAD), place, THETA)
    v = matmul(a, wv).reshape(ROWS, KV_HEADS, HEAD)
    seen = attention(q, k, v).reshape(ROWS, HEADS * HEAD)
    return (x.astype(jnp.float32) + jnp.dot(seen, wo, preferred_element_type=jnp.float32)).astype(jnp.bfloat16)
```

```python
import functools

import jax
import jax.numpy as jnp
import numpy as np
from jax import lax
from jax.experimental import pallas as pl
from jax.experimental.pallas import tpu as pltpu
from jax.sharding import PartitionSpec as P

HEAD = 128
THETA = 10000
NEG = -1e30
HIDDEN = 2 * NEG
LOG2E = 1.4426950408889634
MESH = pl.DeviceIdType.MESH
PIECES = 16
HOP = 2
RING = 4
CHIPS = 4


def _dot(a, b, ca, cb):
    return lax.dot_general(a, b, (((ca,), (cb,)), ((), ())), preferred_element_type=jnp.float32)


def _kernel(n, h, x_hbm, gain_ref, wq, wk, wv, wo, cos_ref, sin_ref, y_hbm, agx, rsp, rsm, rsd,
            xv, nbuf, wqb, wob, xb, acc, qs, seen, kc, vc, top_s, mix_s, term, tsum, dsend, zsend, dbuf, cbuf, ybuf,
            load_sem, wq_sem, wo_sem, nb_sem, y_sem, send_p, send_m, recv_p, recv_m, send_da, recv_da, send_dr, recv_dr):
    R, D = x_hbm.shape
    W = D // n
    Q = 2 * R
    HQ = wq.shape[1]
    H = HQ // HEAD
    N4 = CHIPS * n
    me = lax.axis_index("tp")
    z, c = lax.div(me, 2), lax.rem(me, 2)
    partner = 2 * z + 1 - c
    up = jnp.minimum(me + 2, 2 * CHIPS - 2 + c)
    down = jnp.maximum(me - 2, c)
    lowest, highest = z == 0, z == CHIPS - 1
    not_lowest, not_highest = z >= 1, z <= CHIPS - 2
    mine = pl.ds(pl.multiple_of(c * R, R), R)
    theirs = pl.ds(pl.multiple_of((1 - c) * R, R), R)
    shift = h * jnp.maximum(z, 1) + 1
    late = h * jnp.minimum(z, 1)

    def cols(p):
        return pl.ds(pl.multiple_of(p * W, W), W)

    def remote(src, dst, ssem, rsem, to):
        return pltpu.make_async_remote_copy(src_ref=src, dst_ref=dst, send_sem=ssem, recv_sem=rsem, device_id={"tp": to}, device_id_type=MESH)

    def arrived(dst, rsem, ssem):
        remote(dst, dst, ssem, rsem, partner).wait_recv()

    def chunk_of(s):
        return jnp.where(s - 1 < z, s - 1, s)

    def wq_tile(p, slot):
        rows = pl.ds(pl.multiple_of(p * W, W), W)
        return [pltpu.make_async_copy(wq.at[rows, :], wqb.at[slot, :, pl.ds(0, HQ)], wq_sem.at[slot, 0]),
                pltpu.make_async_copy(wk.at[rows, :], wqb.at[slot, :, pl.ds(HQ, HEAD)], wq_sem.at[slot, 1]),
                pltpu.make_async_copy(wv.at[rows, :], wqb.at[slot, :, pl.ds(HQ + HEAD, HEAD)], wq_sem.at[slot, 2])]

    def wo_tile(p, slot):
        return pltpu.make_async_copy(wo.at[:, cols(p)], wob.at[slot], wo_sem.at[slot])

    for copy in wq_tile(0, 0):
        copy.start()
    wo_tile(0, n % 2).start()
    whole_x = pltpu.make_async_copy(x_hbm, xv, load_sem.at[0])
    whole_x.start()
    barrier = pltpu.get_barrier_semaphore()
    pl.semaphore_signal(barrier, inc=1, device_id={"tp": partner}, device_id_type=MESH)

    @pl.when(not_highest)
    def _():
        pl.semaphore_signal(barrier, inc=1, device_id={"tp": up}, device_id_type=MESH)

    @pl.when(not_lowest)
    def _():
        pl.semaphore_signal(barrier, inc=1, device_id={"tp": down}, device_id_type=MESH)

    whole_x.wait()

    def squares(p, total):
        wide = xv[:, cols(p)].astype(jnp.float32)
        wide = wide * wide
        return total + functools.reduce(jnp.add, [wide[:, i : i + 128] for i in range(0, W, 128)])

    total = lax.fori_loop(0, n, squares, jnp.zeros((R, 128), jnp.float32))
    scale = lax.rsqrt(jnp.sum(total, axis=-1, keepdims=True) * (1.0 / D) + 1e-6)

    def own_piece(p, slot):
        return pltpu.make_async_copy(nbuf.at[slot], agx.at[z, p, mine, :], nb_sem.at[slot])

    def norm_piece(p, _):
        slot = lax.rem(p, 4)

        @pl.when(p >= 4)
        def _():
            own_piece(p - 4, slot).wait()

        nbuf[slot] = (xv[:, cols(p)].astype(jnp.float32) * scale * gain_ref[:, cols(p)].astype(jnp.float32)).astype(jnp.bfloat16)
        own_piece(p, slot).start()

    lax.fori_loop(0, n, norm_piece, None)
    for p in range(n - 4, n):
        own_piece(p, p % 4).wait()
    pl.semaphore_wait(barrier, 1 + (z > 0).astype(jnp.int32) + (z < CHIPS - 1).astype(jnp.int32))

    def hand_over(chunk, p):
        return remote(agx.at[chunk, p, mine, :], agx.at[chunk, p, mine, :], send_da.at[chunk * n + p], recv_da.at[chunk * n + p], partner)

    def own_over(p, _):
        hand_over(z, p).start()

    lax.fori_loop(0, n, own_over, None)

    def sent_up(g):
        remote(zsend.at[0, 0], rsp.at[0, 0], send_p.at[lax.rem(g, RING)], recv_p.at[0], up).wait_send()

    def sent_down(g):
        remote(zsend.at[1, 0], rsm.at[0, 0], send_m.at[lax.rem(g, RING)], recv_m.at[0], down).wait_send()

    def gather_step(t):
        i = t - h * z

        @pl.when((i >= 0) & (i < n * z))
        def _():
            arrived(agx.at[lax.div(i, n), lax.rem(i, n), mine, :], recv_p.at[i], send_p.at[0])

        @pl.when(not_highest & (i >= 0) & (i < n * (z + 1)))
        def _():
            @pl.when(i >= RING)
            def _():
                sent_up(i - RING)

            block = agx.at[lax.div(i, n), lax.rem(i, n), mine, :]
            remote(block, block, send_p.at[lax.rem(i, RING)], recv_p.at[i], up).start()

        @pl.when(not_lowest & (t < n * (CHIPS - z)))
        def _():
            @pl.when(t >= RING)
            def _():
                sent_down(t - RING)

            block = agx.at[z + lax.div(t, n), lax.rem(t, n), mine, :]
            remote(block, block, send_m.at[lax.rem(t, RING)], recv_m.at[t], down).start()

        @pl.when((i >= 0) & (i < n * z))
        def _():
            hand_over(lax.div(i, n), lax.rem(i, n)).start()

        j = t - h

        @pl.when((j >= 0) & (j < n * (CHIPS - 1 - z)))
        def _():
            chunk, p = z + 1 + lax.div(j, n), lax.rem(j, n)
            arrived(agx.at[chunk, p, mine, :], recv_m.at[j], send_m.at[0])
            hand_over(chunk, p).start()

    def turned(t, chunk):
        t = t.astype(jnp.bfloat16).astype(jnp.float32)
        here = pl.ds(pl.multiple_of(chunk * Q, Q), Q)
        return (t * cos_ref[here, :] + pltpu.roll(t, HEAD // 2, 1) * sin_ref[here, :]).astype(jnp.bfloat16)

    def project_end(which, chunk):
        rows = slice(which * Q, which * Q + Q)
        here = pl.ds(pl.multiple_of(chunk * Q, Q), Q)
        for i in range(H):
            qs[which, i * Q : (i + 1) * Q, :] = turned(acc[rows, i * HEAD : (i + 1) * HEAD], chunk)
        kc[here, :] = turned(acc[rows, HQ : HQ + HEAD], chunk)
        vc[here, :] = acc[rows, HQ + HEAD :].astype(jnp.bfloat16)

    columns = H * Q
    wide = min(512, columns)
    strips = range(0, columns, wide)
    e = HEAD**-0.5 * LOG2E

    def attend(which, chunk):
        for at in strips:
            top_s[:, at : at + wide] = jnp.full((1, wide), NEG, jnp.float32)
            mix_s[:, at : at + wide] = jnp.zeros((HEAD + 8, wide), jnp.float32)
        ones = jnp.ones((8, Q), jnp.bfloat16)

        def block(j, masked):
            here = pl.ds(pl.multiple_of(j * Q, Q), Q)
            scores = [_dot(kc[here, :], qs[which, at : at + wide, :], 1, 1) for at in strips]
            if masked:
                seen_by = lax.rem(lax.broadcasted_iota(jnp.int32, (Q, wide), 1), Q) >= lax.broadcasted_iota(jnp.int32, (Q, wide), 0)
            weights, keeps = [], []
            for at, s in zip(strips, scores):
                if masked:
                    s = jnp.where(seen_by, s, HIDDEN)
                old = top_s[:, at : at + wide]
                top = jnp.maximum(old, s.max(axis=0, keepdims=True))
                top_s[:, at : at + wide] = top
                weights.append(jnp.exp2((s - top) * e).astype(jnp.bfloat16))
                keeps.append(jnp.exp2((old - top) * e))
            values = jnp.concatenate([vc[here, :].T, ones], axis=0)
            for at, p, keep in zip(strips, weights, keeps):
                mix_s[:, at : at + wide] = mix_s[:, at : at + wide] * keep + _dot(values, p, 1, 0)

        lax.fori_loop(0, chunk, lambda j, _: block(j, False), None)
        block(chunk, True)
        for i in range(H):
            part = mix_s[:HEAD, i * Q : (i + 1) * Q] * (1 / mix_s[HEAD : HEAD + 1, i * Q : (i + 1) * Q])
            seen[which, :, i * HEAD : (i + 1) * HEAD] = part.T.astype(jnp.bfloat16)

    def step(t, _):
        gather_step(t)
        u = t - shift
        f, p = lax.div(jnp.maximum(u, 0), n), lax.rem(jnp.maximum(u, 0), n)
        projecting = (u >= 0) & (u < 3 * n)
        emitting = (u >= n) & (u < N4)
        chunk = chunk_of(f + 1)
        slot = lax.rem(p + f * n, 2)

        x_load = pltpu.make_async_copy(agx.at[jnp.minimum(chunk, CHIPS - 1), p], xb.at[0], load_sem.at[0])
        own_load = pltpu.make_async_copy(agx.at[z, p], xb.at[1], load_sem.at[1])

        @pl.when(projecting)
        def _():
            place = agx.at[chunk, p, theirs, :]
            arrived(place, recv_da.at[chunk * n + p], send_p.at[0])
            x_load.start()

            @pl.when(f == 0)
            def _():
                arrived(agx.at[z, p, theirs, :], recv_da.at[z * n + p], send_p.at[0])
                own_load.start()

            @pl.when(u + 1 < 3 * n)
            def _():
                for copy in wq_tile(lax.rem(p + 1, n), 1 - slot):
                    copy.start()

        @pl.when(emitting)
        def _():
            wo_tile(p, slot).wait()

            @pl.when(u + 1 < N4)
            def _():
                wo_tile(lax.rem(p + 1, n), 1 - slot).start()

            def emit(which, stage, g):
                for at in range(0, W, 256):
                    to = min(at + 256, W)
                    term[:, at:to] = _dot(seen[which], wob[slot, :, at:to], 1, 0)
                ring = lax.rem(g, RING)
                out = remote(dsend.at[which, ring], rsd.at[stage, p], send_dr.at[which, ring], recv_dr.at[stage * n + p], partner)

                @pl.when(g >= RING)
                def _():
                    out.wait_send()

                dsend[which, ring] = term[theirs, :].astype(jnp.bfloat16)
                out.start()
                tsum[stage, p] = term[mine, :]

            emit(0, f - 1, u - n)

            @pl.when(f == 3)
            def _():
                emit(1, 3, p)

        u1 = u - 1
        pairing = (u1 >= n) & (u1 < N4)
        f1, p1 = lax.div(jnp.maximum(u1, n), n), lax.rem(jnp.maximum(u1, n), n)
        pair_load = pltpu.make_async_copy(rsd.at[f1 - 1, p1], dbuf.at[0], load_sem.at[2])
        pair_own_load = pltpu.make_async_copy(rsd.at[3, p1], dbuf.at[1], load_sem.at[3])

        @pl.when(pairing)
        def _():
            arrived(rsd.at[f1 - 1, p1], recv_dr.at[(f1 - 1) * n + p1], send_p.at[0])
            pair_load.start()

            @pl.when(f1 == 3)
            def _():
                arrived(rsd.at[3, p1], recv_dr.at[3 * n + p1], send_p.at[0])
                pair_own_load.start()

        downward = not_lowest & (u1 >= n * (CHIPS - z)) & (u1 < N4)
        down_load = pltpu.make_async_copy(rsm.at[jnp.maximum(f1 - 2, 0), p1], cbuf.at[1], load_sem.at[5])

        @pl.when(downward & not_highest)
        def _():
            arrived(rsm.at[f1 - 2, p1], recv_m.at[u1 - n], send_p.at[0])
            down_load.start()

        u2 = u1 - late
        upward = not_highest & (u2 >= n * (z + 1)) & (u2 < N4)
        f2, p2 = lax.div(jnp.maximum(u2, n), n), lax.rem(jnp.maximum(u2, n), n)
        up_load = pltpu.make_async_copy(rsp.at[f2 - 1, p2], cbuf.at[0], load_sem.at[4])

        @pl.when(upward & not_lowest)
        def _():
            arrived(rsp.at[f2 - 1, p2], recv_p.at[u2], send_p.at[0])
            up_load.start()

        @pl.when(projecting)
        def _():
            for copy in wq_tile(p, slot):
                copy.wait()

            def project(which):
                rows = slice(which * Q, which * Q + Q)
                for at in range(0, HQ + 2 * HEAD, 256):
                    got = _dot(xb[which], wqb[slot, :, at : at + 256], 1, 0)
                    acc[rows, at : at + 256] = jnp.where(p == 0, got, acc[rows, at : at + 256] + got)

            x_load.wait()
            project(0)

            @pl.when(f == 0)
            def _():
                own_load.wait()
                project(1)

        @pl.when(pairing)
        def _():
            pair_load.wait()
            tsum[f1 - 1, p1] += dbuf[0].astype(jnp.float32)

            @pl.when(f1 == 3)
            def _():
                pair_own_load.wait()
                tsum[3, p1] += dbuf[1].astype(jnp.float32)

        @pl.when(downward)
        def _():
            ring = lax.rem(u1, RING)
            sent_down(u1 - RING)
            here = f1 - CHIPS + z

            @pl.when(not_highest)
            def _():
                down_load.wait()
                zsend[1, ring] = (tsum[here, p1] + cbuf[1].astype(jnp.float32)).astype(jnp.bfloat16)

            @pl.when(highest)
            def _():
                zsend[1, ring] = tsum[here, p1].astype(jnp.bfloat16)

            remote(zsend.at[1, ring], rsm.at[f1 - 1, p1], send_m.at[ring], recv_m.at[u1], down).start()

        @pl.when(upward)
        def _():
            ring = lax.rem(u2, RING)
            sent_up(u2 - RING)

            @pl.when(not_lowest)
            def _():
                up_load.wait()
                zsend[0, ring] = (tsum[f2 - 1, p2] + cbuf[0].astype(jnp.float32)).astype(jnp.bfloat16)

            @pl.when(lowest)
            def _():
                zsend[0, ring] = tsum[f2 - 1, p2].astype(jnp.bfloat16)

            remote(zsend.at[0, ring], rsp.at[f2 - 1, p2], send_p.at[ring], recv_p.at[u2], up).start()

        u3 = u1 - 2 * h

        @pl.when((u3 >= 3 * n) & (u3 < N4))
        def _():
            p3 = lax.rem(u3, n)
            ring = lax.rem(p3, 2)
            from_below = pltpu.make_async_copy(rsp.at[jnp.maximum(z - 1, 0), p3], cbuf.at[2], load_sem.at[6])
            from_above = pltpu.make_async_copy(rsm.at[2, p3], cbuf.at[3], load_sem.at[7])

            @pl.when(not_lowest)
            def _():
                arrived(rsp.at[z - 1, p3], recv_p.at[z * n + p3], send_p.at[0])
                from_below.start()

            @pl.when(not_highest)
            def _():
                arrived(rsm.at[2, p3], recv_m.at[3 * n + p3], send_p.at[0])
                from_above.start()

            @pl.when(not_lowest)
            def _():
                from_below.wait()
                tsum[3, p3] += cbuf[2].astype(jnp.float32)

            @pl.when(not_highest)
            def _():
                from_above.wait()
                tsum[3, p3] += cbuf[3].astype(jnp.float32)

            @pl.when(p3 >= 2)
            def _():
                pltpu.make_async_copy(ybuf.at[ring], y_hbm.at[:, cols(p3 - 2)], y_sem.at[ring]).wait()

            ybuf[ring] = (xv[:, cols(p3)].astype(jnp.float32) + tsum[3, p3]).astype(jnp.bfloat16)
            pltpu.make_async_copy(ybuf.at[ring], y_hbm.at[:, cols(p3)], y_sem.at[ring]).start()

        @pl.when(projecting & (p == n - 1))
        def _():
            project_end(0, chunk)

            @pl.when(f == 0)
            def _():
                project_end(1, z)

            lax.fori_loop(0, jnp.where(f == 2, 2, 1), lambda which, _: attend(which, jnp.where(which == 0, chunk, z)), None)

    lax.fori_loop(0, N4 + 1 + 2 * h + shift, step, None)

    for g in range(N4 - RING, N4):

        @pl.when(not_highest)
        def _():
            sent_up(g)

        @pl.when(not_lowest)
        def _():
            sent_down(g)

    def drain(g, _):
        chunk, p = lax.div(g, n), lax.rem(g, n)
        hand_over(chunk, p).wait_send()

    lax.fori_loop(0, N4, drain, None)
    for which in range(2):
        for ring in range(RING):
            remote(dsend.at[which, ring], rsd.at[0, 0], send_dr.at[which, ring], recv_dr.at[0], partner).wait_send()
    for p in range(n - 2, n):
        pltpu.make_async_copy(ybuf.at[p % 2], y_hbm.at[:, pl.ds(p * W, W)], y_sem.at[p % 2]).wait()


def layer(x, gain, wq, wk, wv, wo, n=PIECES, h=HOP):
    R, D = x.shape
    HQ = wq.shape[1]
    W, Q, H = D // n, 2 * R, HQ // HEAD
    half = HEAD // 2
    place = np.arange(CHIPS * Q, dtype=np.float32)
    angle = place[:, None] * (np.float32(THETA) ** (-np.arange(half, dtype=np.float32) / np.float32(half)))
    cos, sin = np.cos(angle), np.sin(angle)
    cos = jnp.asarray(np.concatenate([cos, cos], 1), jnp.float32)
    sin = jnp.asarray(np.concatenate([-sin, sin], 1), jnp.float32)
    bf, f32 = jnp.bfloat16, jnp.float32
    vmem, anywhere = pl.BlockSpec(memory_space=pltpu.VMEM), pl.BlockSpec(memory_space=pl.ANY)
    V, DMA = pltpu.VMEM, pltpu.SemaphoreType.DMA
    out = pl.pallas_call(
        functools.partial(_kernel, n, h),
        in_specs=[anywhere, vmem, anywhere, anywhere, anywhere, anywhere, vmem, vmem],
        out_specs=[anywhere] * 5,
        out_shape=[
            jax.ShapeDtypeStruct((R, D), bf),
            jax.ShapeDtypeStruct((CHIPS, n, Q, W), bf),
            jax.ShapeDtypeStruct((3, n, R, W), bf),
            jax.ShapeDtypeStruct((3, n, R, W), bf),
            jax.ShapeDtypeStruct((4, n, R, W), bf),
        ],
        scratch_shapes=[
            V((R, D), bf), V((4, R, W), bf), V((2, W, HQ + 2 * HEAD), bf), V((2, HQ, W), bf), V((2, Q, W), bf),
            V((2 * Q, HQ + 2 * HEAD), f32), V((2, H * Q, HEAD), bf), V((2, Q, HQ), bf), V((CHIPS * Q, HEAD), bf), V((CHIPS * Q, HEAD), bf),
            V((1, H * Q), f32), V((HEAD + 8, H * Q), f32), V((Q, W), f32), V((4, n, R, W), f32),
            V((2, RING, R, W), bf), V((2, RING, R, W), bf), V((2, R, W), bf), V((4, R, W), bf), V((2, R, W), bf),
            DMA((8,)), DMA((2, 3)), DMA((2,)), DMA((4,)), DMA((2,)), DMA((RING,)), DMA((RING,)), DMA((CHIPS * n,)), DMA((CHIPS * n,)),
            DMA((CHIPS * n,)), DMA((CHIPS * n,)), DMA((2, RING)), DMA((CHIPS * n,)),
        ],
        compiler_params=pltpu.CompilerParams(collective_id=0, has_side_effects=True, vmem_limit_bytes=66_000_000),
        cost_estimate=pl.CostEstimate(flops=2 * CHIPS * Q * D * (2 * HQ + 2 * HEAD), bytes_accessed=300_000_000, transcendentals=H * (CHIPS * Q) ** 2),
    )(x, gain[None], wq, wk, wv, wo, cos, sin)
    return out[0]


def solution(mesh):
    tokens, columns = P(("dp", "tp"), None), P(None, "tp")
    return jax.shard_map(layer, mesh=mesh, in_specs=(tokens, P(None), columns, columns, columns, P("tp", None)), out_specs=tokens, check_vma=False)
```

```python
import functools

import jax
import jax.numpy as jnp
import numpy as np
from jax import lax
from jax.experimental import pallas as pl
from jax.experimental.pallas import tpu as pltpu
from jax.sharding import PartitionSpec as P

HEAD = 128
THETA = 10000
NEG = -1e30
HIDDEN = 2 * NEG
LOG2E = 1.4426950408889634
MESH = pl.DeviceIdType.MESH
STEPS = 8
HOP = 2
BACK = 4
RING = 4
CHIPS = 4
UNITS = 2 * CHIPS


def _dot(a, b, ca, cb):
    return lax.dot_general(a, b, (((ca,), (cb,)), ((), ())), preferred_element_type=jnp.float32)


def _kernel(n, h, x_hbm, gain_ref, wq, wk, wv, wo, cos_ref, sin_ref, y_hbm, agx, rsp, rsm, rsd, rso, finp, finm,
            gains, xv, wqb, wob, xb, xo, acc, qs, seen, kc, vc, top_s, mix_s, tsum, town, dsend, osend, zsend, dbuf, obuf, cbuf, fbuf, ybuf,
            load_sem, own_sem, wq_sem, wo_sem, y_sem, send_p, send_m, recv_p, recv_m, send_da, recv_da, send_own, recv_own, send_dr, recv_dr,
            send_do, recv_do, recv_fp, recv_fm):
    R, D = x_hbm.shape
    W = D // (2 * n)
    W2 = 2 * W
    HQ = wq.shape[1]
    H = HQ // HEAD
    N2 = 2 * n
    END = UNITS * n
    me = lax.axis_index("tp")
    z, c = lax.div(me, 2), lax.rem(me, 2)
    other = 1 - c
    partner = 2 * z + other
    up = jnp.minimum(me + 2, UNITS - 2 + c)
    down = jnp.maximum(me - 2, c)
    lowest, highest = z == 0, z == CHIPS - 1
    not_lowest, not_highest = z >= 1, z <= CHIPS - 2
    shift = jnp.where(lowest, BACK, h * z) + 1

    def cols(p, size):
        return pl.ds(pl.multiple_of(p * size, size), size)

    def remote(src, dst, ssem, rsem, to):
        return pltpu.make_async_remote_copy(src_ref=src, dst_ref=dst, send_sem=ssem, recv_sem=rsem, device_id={"tp": to}, device_id_type=MESH)

    def arrived(dst, rsem):
        remote(dst, dst, send_p.at[0], rsem, partner).wait_recv()

    def unit_of(s):
        return jnp.where(s < 2 * z, s, s + 2)

    def held(s):
        return jnp.where(s == 5, 2, s)

    def wq_tile(q, slot):
        rows = pl.ds(pl.multiple_of(q * W2, W2), W2)
        return [pltpu.make_async_copy(wq.at[rows, :], wqb.at[slot, :, pl.ds(0, HQ)], wq_sem.at[slot, 0]),
                pltpu.make_async_copy(wk.at[rows, :], wqb.at[slot, :, pl.ds(HQ, HEAD)], wq_sem.at[slot, 1]),
                pltpu.make_async_copy(wv.at[rows, :], wqb.at[slot, :, pl.ds(HQ + HEAD, HEAD)], wq_sem.at[slot, 2])]

    def wo_tile(q, slot):
        return pltpu.make_async_copy(wo.at[:, cols(q, W2)], wob.at[slot], wo_sem.at[slot])

    GROUPS = 4

    def rows_in(i):
        here = pl.ds(i * (D // GROUPS), D // GROUPS)
        return pltpu.make_async_copy(x_hbm.at[:, here], xv.at[:, here], load_sem.at[i])

    for i in range(GROUPS):
        rows_in(i).start()
    barrier = pltpu.get_barrier_semaphore()
    pl.semaphore_signal(barrier, inc=1, device_id={"tp": partner}, device_id_type=MESH)

    @pl.when(not_highest)
    def _():
        for core in range(2):
            pl.semaphore_signal(barrier, inc=1, device_id={"tp": jnp.minimum(2 * z + 2 + core, UNITS - 1)}, device_id_type=MESH)

    @pl.when(not_lowest)
    def _():
        for core in range(2):
            pl.semaphore_signal(barrier, inc=1, device_id={"tp": jnp.maximum(2 * z - 2 + core, 0)}, device_id_type=MESH)

    kc[...] = jnp.zeros_like(kc)
    vc[...] = jnp.zeros_like(vc)
    total = jnp.zeros((R, 128), jnp.float32)
    for i in range(GROUPS):
        rows_in(i).wait()
        if i == GROUPS - 1:
            for copy in wq_tile(0, 0):
                copy.start()
            wo_tile(0, n % 2).start()

        def squares(p, total):
            wide = xv[:, cols(p, W)].astype(jnp.float32)
            wide = wide * wide
            return total + functools.reduce(jnp.add, [wide[:, k : k + 128] for k in range(0, W, 128)])

        total = lax.fori_loop(2 * n // GROUPS * i, 2 * n // GROUPS * (i + 1), squares, total)
    scale = lax.rsqrt(jnp.sum(total, axis=-1, keepdims=True) * (1.0 / D) + 1e-6)
    gains[...] = gain_ref[...].astype(jnp.float32)

    def own_piece(q, half, slot):
        return pltpu.make_async_copy(zsend.at[half, slot], agx.at[me, q, half], own_sem.at[half, slot])

    def own_over(q):
        return remote(agx.at[me, q], agx.at[me, q], send_own.at[q], recv_own.at[q], partner)

    def written(q):
        for half in range(2):
            own_piece(q, half, lax.rem(q, RING)).wait()
        own_over(q).start()

    pl.semaphore_wait(barrier, 1 + 2 * (z > 0).astype(jnp.int32) + 2 * (z < CHIPS - 1).astype(jnp.int32))

    def hand_over(unit, q):
        return remote(agx.at[unit, q, c], agx.at[unit, q, c], send_da.at[unit * n + q], recv_da.at[unit * n + q], partner)

    def sent_up(g):
        remote(zsend.at[0, 0], rsp.at[0, 0], send_p.at[lax.rem(g, RING)], recv_p.at[0], up).wait_send()

    def sent_down(g):
        remote(zsend.at[1, 0], rsm.at[0, 0], send_m.at[lax.rem(g, RING)], recv_m.at[0], down).wait_send()

    def gather_step(t):
        i = t - h * z

        @pl.when(t < n)
        def _():
            arrived(agx.at[partner, t], recv_own.at[t])

        @pl.when((i >= 0) & (i < N2 * z))
        def _():
            arrived(agx.at[lax.div(i, n), lax.rem(i, n), c], recv_p.at[i])

        @pl.when(not_highest & (i >= 0) & (i < N2 * (z + 1)))
        def _():
            @pl.when(i >= RING)
            def _():
                sent_up(i - RING)

            block = agx.at[lax.div(i, n), lax.rem(i, n), c]
            remote(block, block, send_p.at[lax.rem(i, RING)], recv_p.at[i], up).start()

        @pl.when(not_lowest & (t < N2 * (CHIPS - z)))
        def _():
            @pl.when(t >= RING)
            def _():
                sent_down(t - RING)

            block = agx.at[2 * z + lax.div(t, n), lax.rem(t, n), c]
            remote(block, block, send_m.at[lax.rem(t, RING)], recv_m.at[t], down).start()

        @pl.when((i >= 0) & (i < N2 * z))
        def _():
            hand_over(lax.div(i, n), lax.rem(i, n)).start()

        j = t - BACK

        @pl.when((j >= 0) & (j < N2 * (CHIPS - 1 - z)))
        def _():
            unit, q = 2 * z + 2 + lax.div(j, n), lax.rem(j, n)
            arrived(agx.at[unit, q, c], recv_m.at[j])
            hand_over(unit, q).start()

    def norm_piece(q, _):
        slot = lax.rem(q, RING)

        @pl.when(q >= 1)
        def _():
            written(q - 1)

        for half in range(2):
            for k in range(W // 128):
                part = 2 * q * (W // 128) + half * (W // 128) + k
                wide = xv[:, cols(part, 128)].astype(jnp.float32)
                zsend[half, slot, :, k * 128 : (k + 1) * 128] = (wide * scale * gains[pl.ds(part, 1), :]).astype(jnp.bfloat16)
            own_piece(q, half, slot).start()

        @pl.when((q == 3) | (q == 5))
        def _():
            gather_step(lax.div(q - 3, 2))

    lax.fori_loop(0, n, norm_piece, None)
    written(n - 1)

    def turned(t, unit):
        t = t.astype(jnp.bfloat16).astype(jnp.float32)
        here = cols(unit, R)
        return (t * cos_ref[here, :] + pltpu.roll(t, HEAD // 2, 1) * sin_ref[here, :]).astype(jnp.bfloat16)

    def project_end(which, unit):
        rows = slice(which * R, which * R + R)
        here = cols(unit, R)
        for i in range(H):
            qs[which, i * R : (i + 1) * R, :] = turned(acc[rows, i * HEAD : (i + 1) * HEAD], unit)
        kc[here, :] = turned(acc[rows, HQ : HQ + HEAD], unit)
        vc[here, :] = acc[rows, HQ + HEAD :].astype(jnp.bfloat16)

    columns = H * R
    wide = min(512, columns)
    strips = range(0, columns, wide)
    e = HEAD**-0.5 * LOG2E

    def attend(which, unit):
        for at in strips:
            top_s[:, at : at + wide] = jnp.full((1, wide), NEG, jnp.float32)
            mix_s[:, at : at + wide] = jnp.zeros((HEAD + 8, wide), jnp.float32)
        ones = jnp.ones((8, 2 * R), jnp.bfloat16)

        def block(j, masked):
            here = cols(j, 2 * R)
            scores = [_dot(kc[here, :], qs[which, at : at + wide, :], 1, 1) for at in strips]
            if masked:
                place = lax.rem(lax.broadcasted_iota(jnp.int32, (2 * R, wide), 1), R) + lax.rem(unit, 2) * R
                seen_by = place >= lax.broadcasted_iota(jnp.int32, (2 * R, wide), 0)
            weights, keeps = [], []
            for at, s in zip(strips, scores):
                if masked:
                    s = jnp.where(seen_by, s, HIDDEN)
                old = top_s[:, at : at + wide]
                top = jnp.maximum(old, s.max(axis=0, keepdims=True))
                top_s[:, at : at + wide] = top
                weights.append(jnp.exp2((s - top) * e).astype(jnp.bfloat16))
                keeps.append(jnp.exp2((old - top) * e))
            values = jnp.concatenate([vc[here, :].T, ones], axis=0)
            for at, p, keep in zip(strips, weights, keeps):
                mix_s[:, at : at + wide] = mix_s[:, at : at + wide] * keep + _dot(values, p, 1, 0)

        lax.fori_loop(0, lax.div(unit, 2), lambda j, _: block(j, False), None)
        block(lax.div(unit, 2), True)
        for i in range(H):
            part = mix_s[:HEAD, i * R : (i + 1) * R] * (1 / mix_s[HEAD : HEAD + 1, i * R : (i + 1) * R])
            seen[which, :, i * HEAD : (i + 1) * HEAD] = part.T.astype(jnp.bfloat16)

    TILE = min(256, W)

    def step(t, _):
        gather_step(t)
        u = t - shift
        f, q = lax.div(jnp.maximum(u, 0), n), lax.rem(jnp.maximum(u, 0), n)
        projecting = (u >= 0) & (u < 6 * n)
        emitting = (u >= n) & (u < 7 * n)
        last = f == 6
        unit = unit_of(jnp.minimum(f, 5))
        slot = lax.rem(u + 64, 2)

        loads = [pltpu.make_async_copy(agx.at[unit, q, k], xb.at[:, pl.ds(k * W, W)], load_sem.at[k]) for k in range(2)]

        def own_loads(q):
            return [pltpu.make_async_copy(agx.at[2 * z + core, q, k], xo.at[lax.rem(q, 2), pl.ds(core * R, R), pl.ds(k * W, W)],
                                          load_sem.at[2 + 2 * core + k]) for core in range(2) for k in range(2)]

        @pl.when(projecting)
        def _():
            arrived(agx.at[unit, q, other], recv_da.at[unit * n + q])
            for copy in loads:
                copy.start()

        u1 = u - 1
        pairing = (u1 >= n) & (u1 < 7 * n)
        f1, q1 = lax.div(jnp.maximum(u1, n), n), lax.rem(jnp.maximum(u1, n), n)
        s1 = jnp.minimum(f1 - 1, 5)
        pair_load = pltpu.make_async_copy(rsd.at[s1, q1], dbuf, load_sem.at[6])
        pair_own_load = pltpu.make_async_copy(rso.at[q1], obuf, load_sem.at[7])

        @pl.when(pairing)
        def _():
            arrived(rsd.at[s1, q1], recv_dr.at[s1 * n + q1])
            pair_load.start()

            @pl.when(f1 == 6)
            def _():
                arrived(rso.at[q1], recv_do.at[q1])
                pair_own_load.start()

        gd = t
        downward = not_lowest & (gd >= N2 * (CHIPS - z)) & (gd < END)
        qd = lax.rem(gd, n)
        to_d = jnp.clip(lax.div(gd, n) - 2 * (CHIPS - z), 0, 5)
        down_load = pltpu.make_async_copy(rsm.at[jnp.minimum(to_d, 3), qd], cbuf.at[1], load_sem.at[9])
        gu = t - h * z
        upward = not_highest & (gu >= N2 * (z + 1)) & (gu < END)
        qu = lax.rem(jnp.maximum(gu, 0), n)
        to_u = jnp.clip(lax.div(jnp.maximum(gu, 0), n), 2, UNITS - 1)
        up_load = pltpu.make_async_copy(rsp.at[jnp.maximum(to_u - 4, 0), qu], cbuf.at[0], load_sem.at[8])

        @pl.when(downward & not_highest)
        def _():
            arrived(rsm.at[jnp.minimum(to_d, 3), qd], recv_m.at[gd - N2])
            down_load.start()

        @pl.when(upward & not_lowest)
        def _():
            arrived(rsp.at[jnp.maximum(to_u - 4, 0), qu], recv_p.at[gu])
            up_load.start()

        @pl.when(projecting & (u + 1 < 6 * n))
        def _():
            for copy in wq_tile(lax.rem(q + 1, n), 1 - slot):
                copy.start()

        @pl.when(emitting)
        def _():
            wo_tile(q, slot).wait()

            @pl.when(u + 1 < 7 * n)
            def _():
                wo_tile(lax.rem(q + 1, n), 1 - slot).start()

            def term(which, start):
                return _dot(seen[which], wob[slot, :, pl.ds(pl.multiple_of(start, TILE), TILE)], 1, 0)

            g = u - n
            ring = lax.rem(g, RING)
            stage = jnp.minimum(f - 1, 5)
            out = remote(dsend.at[ring], rsd.at[stage, q], send_dr.at[ring], recv_dr.at[stage * n + q], partner)

            @pl.when(g >= RING)
            def _():
                out.wait_send()

            for at in range(0, W, TILE):
                dsend[ring, :, at : at + TILE] = term(0, other * W + at).astype(jnp.bfloat16)
            out.start()
            for at in range(0, W, TILE):
                tsum[held(stage), q, :, at : at + TILE] = term(0, c * W + at)

            @pl.when(last)
            def _():
                ring = lax.rem(q, 2)
                out = remote(osend.at[ring], rso.at[q], send_do.at[ring], recv_do.at[q], partner)

                @pl.when(q >= 2)
                def _():
                    out.wait_send()

                for at in range(0, W2, TILE):
                    osend[ring, :, at : at + TILE] = term(1 + other, at).astype(jnp.bfloat16)
                out.start()
                for at in range(0, W2, TILE):
                    town[q, :, at : at + TILE] = term(1 + c, at)

        @pl.when(pairing)
        def _():
            pair_load.wait()
            tsum[held(s1), q1] += dbuf[...].astype(jnp.float32)

            @pl.when(f1 == 6)
            def _():
                pair_own_load.wait()
                town[q1] += obuf[...].astype(jnp.float32)

        @pl.when(downward)
        def _():
            ring = lax.rem(gd, RING)
            sent_down(gd - RING)

            @pl.when(not_highest)
            def _():
                down_load.wait()
                zsend[1, ring] = (tsum[held(to_d), qd] + cbuf[1].astype(jnp.float32)).astype(jnp.bfloat16)

            @pl.when(highest)
            def _():
                zsend[1, ring] = tsum[held(to_d), qd].astype(jnp.bfloat16)

            @pl.when(to_d >= 2 * z - 2)
            def _():
                remote(zsend.at[1, ring], finm.at[qd, c], send_m.at[ring], recv_fm.at[2 * qd + c], to_d).start()

            @pl.when(to_d < 2 * z - 2)
            def _():
                remote(zsend.at[1, ring], rsm.at[jnp.minimum(to_d, 3), qd], send_m.at[ring], recv_m.at[gd], down).start()

        @pl.when(upward)
        def _():
            ring = lax.rem(gu, RING)
            sent_up(gu - RING)

            @pl.when(not_lowest)
            def _():
                up_load.wait()
                zsend[0, ring] = (tsum[held(to_u - 2), qu] + cbuf[0].astype(jnp.float32)).astype(jnp.bfloat16)

            @pl.when(lowest)
            def _():
                zsend[0, ring] = tsum[held(to_u - 2), qu].astype(jnp.bfloat16)

            @pl.when(to_u < 2 * z + 4)
            def _():
                remote(zsend.at[0, ring], finp.at[qu, c], send_p.at[ring], recv_fp.at[2 * qu + c], to_u).start()

            @pl.when(to_u >= 2 * z + 4)
            def _():
                remote(zsend.at[0, ring], rsp.at[jnp.maximum(to_u - 4, 0), qu], send_p.at[ring], recv_p.at[gu], up).start()

        @pl.when(projecting)
        def _():
            for copy in wq_tile(q, slot):
                copy.wait()

            def project(rows, start):
                for at in range(0, HQ + 2 * HEAD, 256):
                    got = _dot(rows[...], wqb[slot, :, at : at + 256], 1, 0)
                    here = slice(start, start + rows.shape[0])
                    acc[here, at : at + 256] = jnp.where(q == 0, got, acc[here, at : at + 256] + got)

            @pl.when(f == 0)
            def _():
                for copy in own_loads(q):
                    copy.wait()
                project(xo.at[lax.rem(q, 2)], R)

            for copy in loads:
                copy.wait()
            project(xb, 0)

        @pl.when((u + 1 >= 0) & (u + 1 < n))
        def _():
            for copy in own_loads(jnp.maximum(u + 1, 0)):
                copy.start()

        u3 = u - 1 + 2 * c

        @pl.when((u3 >= (6 + c) * n) & (u3 < (7 + c) * n))
        def _():
            q3 = lax.rem(u3, n)
            ring = lax.rem(q3, 2)
            for k in range(2):
                from_below = pltpu.make_async_copy(finp.at[q3, k], fbuf.at[0, k], load_sem.at[10 + k])
                from_above = pltpu.make_async_copy(finm.at[q3, k], fbuf.at[1, k], load_sem.at[12 + k])

                @pl.when(not_lowest)
                def _():
                    arrived(finp.at[q3, k], recv_fp.at[2 * q3 + k])
                    from_below.start()

                @pl.when(not_highest)
                def _():
                    arrived(finm.at[q3, k], recv_fm.at[2 * q3 + k])
                    from_above.start()

            @pl.when(q3 >= 2)
            def _():
                pltpu.make_async_copy(ybuf.at[ring], y_hbm.at[:, cols(q3 - 2, W2)], y_sem.at[ring]).wait()

            for k in range(2):
                half = slice(k * W, k * W + W)

                @pl.when(not_lowest)
                def _():
                    pltpu.make_async_copy(finp.at[q3, k], fbuf.at[0, k], load_sem.at[10 + k]).wait()
                    town[q3, :, half] += fbuf[0, k].astype(jnp.float32)

                @pl.when(not_highest)
                def _():
                    pltpu.make_async_copy(finm.at[q3, k], fbuf.at[1, k], load_sem.at[12 + k]).wait()
                    town[q3, :, half] += fbuf[1, k].astype(jnp.float32)

            ybuf[ring] = (xv[:, cols(q3, W2)].astype(jnp.float32) + town[q3]).astype(jnp.bfloat16)
            pltpu.make_async_copy(ybuf.at[ring], y_hbm.at[:, cols(q3, W2)], y_sem.at[ring]).start()

        @pl.when(projecting & (q == n - 1))
        def _():
            project_end(0, unit)

            @pl.when(f == 0)
            def _():
                project_end(1, 2 * z)
                project_end(2, 2 * z + 1)

            lax.fori_loop(0, jnp.where(f == 5, 3, 1), lambda which, _: attend(which, jnp.where(which == 0, unit, 2 * z + which - 1)), None)

    lax.fori_loop(2, END + shift, step, None)

    for g in range(END - RING, END):

        @pl.when(not_highest)
        def _():
            sent_up(g)

        @pl.when(not_lowest)
        def _():
            sent_down(g)

    def drain(g, _):
        unit, q = lax.div(g, n), lax.rem(g, n)

        @pl.when(lax.div(unit, 2) != z)
        def _():
            hand_over(unit, q).wait_send()

    lax.fori_loop(0, END, drain, None)

    def drain_own(q, _):
        own_over(q).wait_send()

    lax.fori_loop(0, n, drain_own, None)
    for ring in range(RING):
        remote(dsend.at[ring], rsd.at[0, 0], send_dr.at[ring], recv_dr.at[0], partner).wait_send()
    for ring in range(2):
        remote(osend.at[ring], rso.at[0], send_do.at[ring], recv_do.at[0], partner).wait_send()
        q = n - 2 + ring
        pltpu.make_async_copy(ybuf.at[q % 2], y_hbm.at[:, pl.ds(q * W2, W2)], y_sem.at[q % 2]).wait()


def layer(x, gain, wq, wk, wv, wo, n=STEPS, h=HOP):
    R, D = x.shape
    HQ = wq.shape[1]
    W, H = D // (2 * n), HQ // HEAD
    half = HEAD // 2
    place = np.arange(UNITS * R, dtype=np.float32)
    angle = place[:, None] * (np.float32(THETA) ** (-np.arange(half, dtype=np.float32) / np.float32(half)))
    cos, sin = np.cos(angle), np.sin(angle)
    cos = jnp.asarray(np.concatenate([cos, cos], 1), jnp.float32)
    sin = jnp.asarray(np.concatenate([-sin, sin], 1), jnp.float32)
    bf, f32 = jnp.bfloat16, jnp.float32
    vmem, anywhere = pl.BlockSpec(memory_space=pltpu.VMEM), pl.BlockSpec(memory_space=pl.ANY)
    V, DMA = pltpu.VMEM, pltpu.SemaphoreType.DMA
    places = [(R, D), (UNITS, n, 2, R, W), (4, n, R, W), (4, n, R, W), (6, n, R, W), (n, R, 2 * W), (n, 2, R, W), (n, 2, R, W)]
    out = pl.pallas_call(
        functools.partial(_kernel, n, h),
        in_specs=[anywhere, vmem, anywhere, anywhere, anywhere, anywhere, vmem, vmem],
        out_specs=[anywhere] * len(places),
        out_shape=[jax.ShapeDtypeStruct(shape, bf) for shape in places],
        scratch_shapes=[
            V((D // 128, 128), f32), V((R, D), bf), V((2, 2 * W, HQ + 2 * HEAD), bf), V((2, HQ, 2 * W), bf), V((R, 2 * W), bf), V((2, 2 * R, 2 * W), bf),
            V((3 * R, HQ + 2 * HEAD), f32), V((3, H * R, HEAD), bf), V((3, R, HQ), bf), V((UNITS * R, HEAD), bf), V((UNITS * R, HEAD), bf),
            V((1, H * R), f32), V((HEAD + 8, H * R), f32), V((5, n, R, W), f32), V((n, R, 2 * W), f32),
            V((RING, R, W), bf), V((2, R, 2 * W), bf), V((2, RING, R, W), bf), V((R, W), bf), V((R, 2 * W), bf), V((2, R, W), bf),
            V((2, 2, R, W), bf), V((2, R, 2 * W), bf),
            DMA((14,)), DMA((2, RING)), DMA((2, 3)), DMA((2,)), DMA((2,)), DMA((RING,)), DMA((RING,)), DMA((UNITS * n,)), DMA((UNITS * n,)),
            DMA((UNITS * n,)), DMA((UNITS * n,)), DMA((n,)), DMA((n,)), DMA((RING,)), DMA((6 * n,)),
            DMA((2,)), DMA((n,)), DMA((2 * n,)), DMA((2 * n,)),
        ],
        compiler_params=pltpu.CompilerParams(collective_id=0, has_side_effects=True, vmem_limit_bytes=67_000_000),
        cost_estimate=pl.CostEstimate(flops=2 * UNITS * R * D * (2 * HQ + 2 * HEAD), bytes_accessed=800_000_000, transcendentals=H * (UNITS * R) ** 2),
    )(x, gain.reshape(D // 128, 128), wq, wk, wv, wo, cos, sin)
    return out[0]


def solution(mesh):
    tokens, columns = P(("dp", "tp"), None), P(None, "tp")
    return jax.shard_map(layer, mesh=mesh, in_specs=(tokens, P(None), columns, columns, columns, P("tp", None)), out_specs=tokens, check_vma=False)
```

```python
import functools

import jax
import jax.numpy as jnp
import numpy as np
from jax import lax
from jax.experimental import pallas as pl
from jax.experimental.pallas import tpu as pltpu
from jax.sharding import PartitionSpec as P

HEAD = 128
THETA = 10000
NEG = -1e30
HIDDEN = 2 * NEG
LOG2E = 1.4426950408889634
MESH = pl.DeviceIdType.MESH
STEPS = 8
HOP = 2
BACK = 4
RING = 4
OWN = 2
CHIPS = 4
UNITS = 2 * CHIPS


def _dot(a, b, ca, cb):
    return lax.dot_general(a, b, (((ca,), (cb,)), ((), ())), preferred_element_type=jnp.float32)


def _kernel(n, h, x_hbm, gain_ref, wq, wk, wv, wo, cos_ref, sin_ref, y_hbm, agx, rsp, rsm, rsd, rso, finp, finm,
            gains, xv, wqb, wob, xb, xo, acc, qs, seen, kc, vc, top_s, mix_s, tsum, town, dsend, osend, zsend, dbuf, obuf, cbuf, fbuf, ybuf,
            load_sem, own_sem, wq_sem, wo_sem, y_sem, send_p, send_m, recv_p, recv_m, send_da, recv_da, send_own, recv_own, send_dr, recv_dr,
            send_do, recv_do, recv_fp, recv_fm):
    R, D = x_hbm.shape
    W = D // (2 * n)
    W2 = 2 * W
    HQ = wq.shape[1]
    H = HQ // HEAD
    N2 = 2 * n
    END = UNITS * n
    me = lax.axis_index("tp")
    z, c = lax.div(me, 2), lax.rem(me, 2)
    other = 1 - c
    partner = 2 * z + other
    up = jnp.minimum(me + 2, UNITS - 2 + c)
    down = jnp.maximum(me - 2, c)
    lowest, highest = z == 0, z == CHIPS - 1
    not_lowest, not_highest = z >= 1, z <= CHIPS - 2
    shift = jnp.where(lowest, BACK, h * z) + 1

    def cols(p, size):
        return pl.ds(pl.multiple_of(p * size, size), size)

    def remote(src, dst, ssem, rsem, to):
        return pltpu.make_async_remote_copy(src_ref=src, dst_ref=dst, send_sem=ssem, recv_sem=rsem, device_id={"tp": to}, device_id_type=MESH)

    def arrived(dst, rsem):
        remote(dst, dst, send_p.at[0], rsem, partner).wait_recv()

    def unit_of(s):
        return jnp.where(s < 2 * z, s, s + 2)

    def held(s):
        return jnp.where(s == 5, 2, s)

    def wq_tile(q, slot):
        rows = pl.ds(pl.multiple_of(q * W2, W2), W2)
        return [pltpu.make_async_copy(wq.at[rows, :], wqb.at[slot, :, pl.ds(0, HQ)], wq_sem.at[slot, 0]),
                pltpu.make_async_copy(wk.at[rows, :], wqb.at[slot, :, pl.ds(HQ, HEAD)], wq_sem.at[slot, 1]),
                pltpu.make_async_copy(wv.at[rows, :], wqb.at[slot, :, pl.ds(HQ + HEAD, HEAD)], wq_sem.at[slot, 2])]

    def wo_tile(q, slot):
        return pltpu.make_async_copy(wo.at[:, cols(q, W2)], wob.at[slot], wo_sem.at[slot])

    GROUPS = 4

    def rows_in(i):
        here = pl.ds(i * (D // GROUPS), D // GROUPS)
        return pltpu.make_async_copy(x_hbm.at[:, here], xv.at[:, here], load_sem.at[i])

    for i in range(GROUPS):
        rows_in(i).start()
    barrier = pltpu.get_barrier_semaphore()
    pl.semaphore_signal(barrier, inc=1, device_id={"tp": partner}, device_id_type=MESH)

    @pl.when(not_highest)
    def _():
        for core in range(2):
            pl.semaphore_signal(barrier, inc=1, device_id={"tp": jnp.minimum(2 * z + 2 + core, UNITS - 1)}, device_id_type=MESH)

    @pl.when(not_lowest)
    def _():
        for core in range(2):
            pl.semaphore_signal(barrier, inc=1, device_id={"tp": jnp.maximum(2 * z - 2 + core, 0)}, device_id_type=MESH)

    kc[...] = jnp.zeros_like(kc)
    vc[...] = jnp.zeros_like(vc)
    total = jnp.zeros((R, 128), jnp.float32)
    for i in range(GROUPS):
        rows_in(i).wait()
        if i == GROUPS - 1:
            for copy in wq_tile(0, 0):
                copy.start()
            wo_tile(0, n % 2).start()

        def squares(p, total):
            wide = xv[:, cols(p, W)].astype(jnp.float32)
            wide = wide * wide
            return total + functools.reduce(jnp.add, [wide[:, k : k + 128] for k in range(0, W, 128)])

        total = lax.fori_loop(2 * n // GROUPS * i, 2 * n // GROUPS * (i + 1), squares, total)
    scale = lax.rsqrt(jnp.sum(total, axis=-1, keepdims=True) * (1.0 / D) + 1e-6)
    gains[...] = gain_ref[...].astype(jnp.float32)

    def own_piece(q, half, slot):
        return pltpu.make_async_copy(zsend.at[half, slot], agx.at[me, q, half], own_sem.at[half, slot])

    def own_over(q):
        return remote(agx.at[me, q], agx.at[me, q], send_own.at[q], recv_own.at[q], partner)

    def written(q):
        for half in range(2):
            own_piece(q, half, lax.rem(q, RING)).wait()
        own_over(q).start()

    pl.semaphore_wait(barrier, 1 + 2 * (z > 0).astype(jnp.int32) + 2 * (z < CHIPS - 1).astype(jnp.int32))

    def hand_over(unit, q):
        return remote(agx.at[unit, q, c], agx.at[unit, q, c], send_da.at[unit * n + q], recv_da.at[unit * n + q], partner)

    def sent_up(g):
        remote(zsend.at[0, 0], rsp.at[0, 0], send_p.at[lax.rem(g, RING)], recv_p.at[0], up).wait_send()

    def sent_down(g):
        remote(zsend.at[1, 0], rsm.at[0, 0], send_m.at[lax.rem(g, RING)], recv_m.at[0], down).wait_send()

    def gather_step(t):
        i = t - h * z

        @pl.when(t < n)
        def _():
            arrived(agx.at[partner, t], recv_own.at[t])

        @pl.when((i >= 0) & (i < N2 * z))
        def _():
            arrived(agx.at[lax.div(i, n), lax.rem(i, n), c], recv_p.at[i])

        @pl.when(not_highest & (i >= 0) & (i < N2 * (z + 1)))
        def _():
            @pl.when(i >= RING)
            def _():
                sent_up(i - RING)

            block = agx.at[lax.div(i, n), lax.rem(i, n), c]
            remote(block, block, send_p.at[lax.rem(i, RING)], recv_p.at[i], up).start()

        @pl.when(not_lowest & (t < N2 * (CHIPS - z)))
        def _():
            @pl.when(t >= RING)
            def _():
                sent_down(t - RING)

            block = agx.at[2 * z + lax.div(t, n), lax.rem(t, n), c]
            remote(block, block, send_m.at[lax.rem(t, RING)], recv_m.at[t], down).start()

        @pl.when((i >= 0) & (i < N2 * z))
        def _():
            hand_over(lax.div(i, n), lax.rem(i, n)).start()

        j = t - BACK

        @pl.when((j >= 0) & (j < N2 * (CHIPS - 1 - z)))
        def _():
            unit, q = 2 * z + 2 + lax.div(j, n), lax.rem(j, n)
            arrived(agx.at[unit, q, c], recv_m.at[j])
            hand_over(unit, q).start()

    def norm_piece(q, _):
        slot = lax.rem(q, RING)

        @pl.when(q >= 3)
        def _():
            written(q - 3)

        for half in range(2):
            for k in range(W // 128):
                part = 2 * q * (W // 128) + half * (W // 128) + k
                wide = xv[:, cols(part, 128)].astype(jnp.float32)
                zsend[half, slot, :, k * 128 : (k + 1) * 128] = (wide * scale * gains[pl.ds(part, 1), :]).astype(jnp.bfloat16)
            own_piece(q, half, slot).start()

    lax.fori_loop(0, n, norm_piece, None)
    for q in range(n - 3, n):
        written(q)

    def turned(t, unit):
        t = t.astype(jnp.bfloat16).astype(jnp.float32)
        here = cols(unit, R)
        return (t * cos_ref[here, :] + pltpu.roll(t, HEAD // 2, 1) * sin_ref[here, :]).astype(jnp.bfloat16)

    def project_end(which, unit):
        rows = slice(which * R, which * R + R)
        here = cols(unit, R)
        for i in range(H):
            qs[which, i * R : (i + 1) * R, :] = turned(acc[rows, i * HEAD : (i + 1) * HEAD], unit)
        kc[here, :] = turned(acc[rows, HQ : HQ + HEAD], unit)
        vc[here, :] = acc[rows, HQ + HEAD :].astype(jnp.bfloat16)

    columns = H * R
    wide = min(512, columns)
    strips = range(0, columns, wide)
    e = HEAD**-0.5 * LOG2E

    def attend(which, unit):
        for at in strips:
            top_s[:, at : at + wide] = jnp.full((1, wide), NEG, jnp.float32)
            mix_s[:, at : at + wide] = jnp.zeros((HEAD + 8, wide), jnp.float32)
        ones = jnp.ones((8, 2 * R), jnp.bfloat16)

        def block(j, masked):
            here = cols(j, 2 * R)
            scores = [_dot(kc[here, :], qs[which, at : at + wide, :], 1, 1) for at in strips]
            if masked:
                place = lax.rem(lax.broadcasted_iota(jnp.int32, (2 * R, wide), 1), R) + lax.rem(unit, 2) * R
                seen_by = place >= lax.broadcasted_iota(jnp.int32, (2 * R, wide), 0)
            weights, keeps = [], []
            for at, s in zip(strips, scores):
                if masked:
                    s = jnp.where(seen_by, s, HIDDEN)
                old = top_s[:, at : at + wide]
                top = jnp.maximum(old, s.max(axis=0, keepdims=True))
                top_s[:, at : at + wide] = top
                weights.append(jnp.exp2((s - top) * e).astype(jnp.bfloat16))
                keeps.append(jnp.exp2((old - top) * e))
            values = jnp.concatenate([vc[here, :].T, ones], axis=0)
            for at, p, keep in zip(strips, weights, keeps):
                mix_s[:, at : at + wide] = mix_s[:, at : at + wide] * keep + _dot(values, p, 1, 0)

        lax.fori_loop(0, lax.div(unit, 2), lambda j, _: block(j, False), None)
        block(lax.div(unit, 2), True)
        for i in range(H):
            part = mix_s[:HEAD, i * R : (i + 1) * R] * (1 / mix_s[HEAD : HEAD + 1, i * R : (i + 1) * R])
            seen[which, :, i * HEAD : (i + 1) * HEAD] = part.T.astype(jnp.bfloat16)

    TILE = min(256, W)

    def step(t, _):
        gather_step(t)
        u = t - shift
        f, q = lax.div(jnp.maximum(u, 0), n), lax.rem(jnp.maximum(u, 0), n)
        projecting = (u >= 0) & (u < 6 * n)
        emitting = (u >= n) & (u < 7 * n)
        own = u - 6 * n - OWN
        closing = (own >= 0) & (own < n)
        qo = jnp.clip(own, 0, n - 1)
        own_slot = lax.rem(qo, 2)

        def own_tile(q, slot):
            return pltpu.make_async_copy(wo.at[:, cols(q, W2)], wqb.at[slot, :, pl.ds(0, W2)], wq_sem.at[slot, 0])

        unit = unit_of(jnp.minimum(f, 5))
        slot = lax.rem(u + 64, 2)

        loads = [pltpu.make_async_copy(agx.at[unit, q, k], xb.at[:, pl.ds(k * W, W)], load_sem.at[k]) for k in range(2)]

        def own_loads(q):
            return [pltpu.make_async_copy(agx.at[2 * z + core, q, k], xo.at[lax.rem(q, 2), pl.ds(core * R, R), pl.ds(k * W, W)],
                                          load_sem.at[2 + 2 * core + k]) for core in range(2) for k in range(2)]

        @pl.when(projecting)
        def _():
            arrived(agx.at[unit, q, other], recv_da.at[unit * n + q])
            for copy in loads:
                copy.start()

        u1 = u - 1
        pairing = (u1 >= n) & (u1 < 7 * n)
        f1, q1 = lax.div(jnp.maximum(u1, n), n), lax.rem(jnp.maximum(u1, n), n)
        s1 = jnp.minimum(f1 - 1, 5)
        pair_load = pltpu.make_async_copy(rsd.at[s1, q1], dbuf, load_sem.at[6])
        pairing_own = (own >= 1) & (own < n + 1)
        qp = jnp.clip(own - 1, 0, n - 1)
        pair_own_load = pltpu.make_async_copy(rso.at[qp], obuf, load_sem.at[7])

        @pl.when(pairing)
        def _():
            arrived(rsd.at[s1, q1], recv_dr.at[s1 * n + q1])
            pair_load.start()

        @pl.when(pairing_own)
        def _():
            arrived(rso.at[qp], recv_do.at[qp])
            pair_own_load.start()

        gd = t
        downward = not_lowest & (gd >= N2 * (CHIPS - z)) & (gd < END)
        qd = lax.rem(gd, n)
        to_d = jnp.clip(lax.div(gd, n) - 2 * (CHIPS - z), 0, 5)
        down_load = pltpu.make_async_copy(rsm.at[jnp.minimum(to_d, 3), qd], cbuf.at[1], load_sem.at[9])
        gu = t - h * z
        upward = not_highest & (gu >= N2 * (z + 1)) & (gu < END)
        qu = lax.rem(jnp.maximum(gu, 0), n)
        to_u = jnp.clip(lax.div(jnp.maximum(gu, 0), n), 2, UNITS - 1)
        up_load = pltpu.make_async_copy(rsp.at[jnp.maximum(to_u - 4, 0), qu], cbuf.at[0], load_sem.at[8])

        @pl.when(downward & not_highest)
        def _():
            arrived(rsm.at[jnp.minimum(to_d, 3), qd], recv_m.at[gd - N2])
            down_load.start()

        @pl.when(upward & not_lowest)
        def _():
            arrived(rsp.at[jnp.maximum(to_u - 4, 0), qu], recv_p.at[gu])
            up_load.start()

        @pl.when(projecting & (u + 1 < 6 * n))
        def _():
            for copy in wq_tile(lax.rem(q + 1, n), 1 - slot):
                copy.start()

        @pl.when(emitting)
        def _():
            wo_tile(q, slot).wait()

            @pl.when(u + 1 < 7 * n)
            def _():
                wo_tile(lax.rem(q + 1, n), 1 - slot).start()

            def term(which, start):
                return _dot(seen[which], wob[slot, :, pl.ds(pl.multiple_of(start, TILE), TILE)], 1, 0)

            g = u - n
            ring = lax.rem(g, RING)
            stage = jnp.minimum(f - 1, 5)
            out = remote(dsend.at[ring], rsd.at[stage, q], send_dr.at[ring], recv_dr.at[stage * n + q], partner)

            @pl.when(g >= RING)
            def _():
                out.wait_send()

            for at in range(0, W, TILE):
                dsend[ring, :, at : at + TILE] = term(0, other * W + at).astype(jnp.bfloat16)
            out.start()
            for at in range(0, W, TILE):
                tsum[held(stage), q, :, at : at + TILE] = term(0, c * W + at)

        @pl.when((own >= -1) & (own + 1 < n))
        def _():
            own_tile(jnp.maximum(own + 1, 0), lax.rem(jnp.maximum(own + 1, 0), 2)).start()

        @pl.when(closing)
        def _():
            own_tile(qo, own_slot).wait()
            ring = lax.rem(qo, 2)
            out = remote(osend.at[ring], rso.at[qo], send_do.at[ring], recv_do.at[qo], partner)

            @pl.when(qo >= 2)
            def _():
                out.wait_send()

            for at in range(0, W2, TILE):
                osend[ring, :, at : at + TILE] = _dot(seen[1 + other], wqb[own_slot, :, at : at + TILE], 1, 0).astype(jnp.bfloat16)
            out.start()
            for at in range(0, W2, TILE):
                town[qo, :, at : at + TILE] = _dot(seen[1 + c], wqb[own_slot, :, at : at + TILE], 1, 0)

        @pl.when(pairing)
        def _():
            pair_load.wait()
            tsum[held(s1), q1] += dbuf[...].astype(jnp.float32)

        @pl.when(pairing_own)
        def _():
            pair_own_load.wait()
            town[qp] += obuf[...].astype(jnp.float32)

        @pl.when(downward)
        def _():
            ring = lax.rem(gd, RING)
            sent_down(gd - RING)

            @pl.when(not_highest)
            def _():
                down_load.wait()
                zsend[1, ring] = (tsum[held(to_d), qd] + cbuf[1].astype(jnp.float32)).astype(jnp.bfloat16)

            @pl.when(highest)
            def _():
                zsend[1, ring] = tsum[held(to_d), qd].astype(jnp.bfloat16)

            @pl.when(to_d >= 2 * z - 2)
            def _():
                remote(zsend.at[1, ring], finm.at[qd, c], send_m.at[ring], recv_fm.at[2 * qd + c], to_d).start()

            @pl.when(to_d < 2 * z - 2)
            def _():
                remote(zsend.at[1, ring], rsm.at[jnp.minimum(to_d, 3), qd], send_m.at[ring], recv_m.at[gd], down).start()

        @pl.when(upward)
        def _():
            ring = lax.rem(gu, RING)
            sent_up(gu - RING)

            @pl.when(not_lowest)
            def _():
                up_load.wait()
                zsend[0, ring] = (tsum[held(to_u - 2), qu] + cbuf[0].astype(jnp.float32)).astype(jnp.bfloat16)

            @pl.when(lowest)
            def _():
                zsend[0, ring] = tsum[held(to_u - 2), qu].astype(jnp.bfloat16)

            @pl.when(to_u < 2 * z + 4)
            def _():
                remote(zsend.at[0, ring], finp.at[qu, c], send_p.at[ring], recv_fp.at[2 * qu + c], to_u).start()

            @pl.when(to_u >= 2 * z + 4)
            def _():
                remote(zsend.at[0, ring], rsp.at[jnp.maximum(to_u - 4, 0), qu], send_p.at[ring], recv_p.at[gu], up).start()

        @pl.when(projecting)
        def _():
            for copy in wq_tile(q, slot):
                copy.wait()

            def project(rows, start):
                for at in range(0, HQ + 2 * HEAD, 256):
                    got = _dot(rows[...], wqb[slot, :, at : at + 256], 1, 0)
                    here = slice(start, start + rows.shape[0])
                    acc[here, at : at + 256] = jnp.where(q == 0, got, acc[here, at : at + 256] + got)

            @pl.when(f == 0)
            def _():
                for copy in own_loads(q):
                    copy.wait()
                project(xo.at[lax.rem(q, 2)], R)

            for copy in loads:
                copy.wait()
            project(xb, 0)

        @pl.when((u + 1 >= 0) & (u + 1 < n))
        def _():
            for copy in own_loads(jnp.maximum(u + 1, 0)):
                copy.start()

        u3 = jnp.where(c == 0, u - 1 - OWN, u + 1)

        @pl.when((u3 >= (6 + c) * n) & (u3 < (7 + c) * n))
        def _():
            q3 = lax.rem(u3, n)
            ring = lax.rem(q3, 2)
            for k in range(2):
                from_below = pltpu.make_async_copy(finp.at[q3, k], fbuf.at[0, k], load_sem.at[10 + k])
                from_above = pltpu.make_async_copy(finm.at[q3, k], fbuf.at[1, k], load_sem.at[12 + k])

                @pl.when(not_lowest)
                def _():
                    arrived(finp.at[q3, k], recv_fp.at[2 * q3 + k])
                    from_below.start()

                @pl.when(not_highest)
                def _():
                    arrived(finm.at[q3, k], recv_fm.at[2 * q3 + k])
                    from_above.start()

            @pl.when(q3 >= 2)
            def _():
                pltpu.make_async_copy(ybuf.at[ring], y_hbm.at[:, cols(q3 - 2, W2)], y_sem.at[ring]).wait()

            for k in range(2):
                half = slice(k * W, k * W + W)

                @pl.when(not_lowest)
                def _():
                    pltpu.make_async_copy(finp.at[q3, k], fbuf.at[0, k], load_sem.at[10 + k]).wait()
                    town[q3, :, half] += fbuf[0, k].astype(jnp.float32)

                @pl.when(not_highest)
                def _():
                    pltpu.make_async_copy(finm.at[q3, k], fbuf.at[1, k], load_sem.at[12 + k]).wait()
                    town[q3, :, half] += fbuf[1, k].astype(jnp.float32)

            ybuf[ring] = (xv[:, cols(q3, W2)].astype(jnp.float32) + town[q3]).astype(jnp.bfloat16)
            pltpu.make_async_copy(ybuf.at[ring], y_hbm.at[:, cols(q3, W2)], y_sem.at[ring]).start()

        @pl.when(projecting & (q == n - 1))
        def _():
            project_end(0, unit)

            @pl.when(f == 0)
            def _():
                project_end(1, 2 * z)
                project_end(2, 2 * z + 1)

        turn = jnp.maximum(u - 6 * n + 1, 0)

        @pl.when((projecting & (q == n - 1)) | ((u >= 6 * n) & (u < 6 * n + 2)))
        def _():
            attend(turn, jnp.where(turn == 0, unit, 2 * z + turn - 1))

    lax.fori_loop(0, END + shift, step, None)

    for g in range(END - RING, END):

        @pl.when(not_highest)
        def _():
            sent_up(g)

        @pl.when(not_lowest)
        def _():
            sent_down(g)

    def drain(g, _):
        unit, q = lax.div(g, n), lax.rem(g, n)

        @pl.when(lax.div(unit, 2) != z)
        def _():
            hand_over(unit, q).wait_send()

    lax.fori_loop(0, END, drain, None)

    def drain_own(q, _):
        own_over(q).wait_send()

    lax.fori_loop(0, n, drain_own, None)
    for ring in range(RING):
        remote(dsend.at[ring], rsd.at[0, 0], send_dr.at[ring], recv_dr.at[0], partner).wait_send()
    for ring in range(2):
        remote(osend.at[ring], rso.at[0], send_do.at[ring], recv_do.at[0], partner).wait_send()
        q = n - 2 + ring
        pltpu.make_async_copy(ybuf.at[q % 2], y_hbm.at[:, pl.ds(q * W2, W2)], y_sem.at[q % 2]).wait()


def layer(x, gain, wq, wk, wv, wo, n=STEPS, h=HOP):
    R, D = x.shape
    HQ = wq.shape[1]
    W, H = D // (2 * n), HQ // HEAD
    half = HEAD // 2
    place = np.arange(UNITS * R, dtype=np.float32)
    angle = place[:, None] * (np.float32(THETA) ** (-np.arange(half, dtype=np.float32) / np.float32(half)))
    cos, sin = np.cos(angle), np.sin(angle)
    cos = jnp.asarray(np.concatenate([cos, cos], 1), jnp.float32)
    sin = jnp.asarray(np.concatenate([-sin, sin], 1), jnp.float32)
    bf, f32 = jnp.bfloat16, jnp.float32
    vmem, anywhere = pl.BlockSpec(memory_space=pltpu.VMEM), pl.BlockSpec(memory_space=pl.ANY)
    V, DMA = pltpu.VMEM, pltpu.SemaphoreType.DMA
    places = [(R, D), (UNITS, n, 2, R, W), (4, n, R, W), (4, n, R, W), (6, n, R, W), (n, R, 2 * W), (n, 2, R, W), (n, 2, R, W)]
    out = pl.pallas_call(
        functools.partial(_kernel, n, h),
        in_specs=[anywhere, vmem, anywhere, anywhere, anywhere, anywhere, vmem, vmem],
        out_specs=[anywhere] * len(places),
        out_shape=[jax.ShapeDtypeStruct(shape, bf) for shape in places],
        scratch_shapes=[
            V((D // 128, 128), f32), V((R, D), bf), V((2, 2 * W, HQ + 2 * HEAD), bf), V((2, HQ, 2 * W), bf), V((R, 2 * W), bf), V((2, 2 * R, 2 * W), bf),
            V((3 * R, HQ + 2 * HEAD), f32), V((3, H * R, HEAD), bf), V((3, R, HQ), bf), V((UNITS * R, HEAD), bf), V((UNITS * R, HEAD), bf),
            V((1, H * R), f32), V((HEAD + 8, H * R), f32), V((5, n, R, W), f32), V((n, R, 2 * W), f32),
            V((RING, R, W), bf), V((2, R, 2 * W), bf), V((2, RING, R, W), bf), V((R, W), bf), V((R, 2 * W), bf), V((2, R, W), bf),
            V((2, 2, R, W), bf), V((2, R, 2 * W), bf),
            DMA((14,)), DMA((2, RING)), DMA((2, 3)), DMA((2,)), DMA((2,)), DMA((RING,)), DMA((RING,)), DMA((UNITS * n,)), DMA((UNITS * n,)),
            DMA((UNITS * n,)), DMA((UNITS * n,)), DMA((n,)), DMA((n,)), DMA((RING,)), DMA((6 * n,)),
            DMA((2,)), DMA((n,)), DMA((2 * n,)), DMA((2 * n,)),
        ],
        compiler_params=pltpu.CompilerParams(collective_id=0, has_side_effects=True, vmem_limit_bytes=67_000_000),
        cost_estimate=pl.CostEstimate(flops=2 * UNITS * R * D * (2 * HQ + 2 * HEAD), bytes_accessed=800_000_000, transcendentals=H * (UNITS * R) ** 2),
    )(x, gain.reshape(D // 128, 128), wq, wk, wv, wo, cos, sin)
    def move(src, dst, held, came, went):
        into = [pltpu.make_async_copy(src.at[:, i * (D // n) : (i + 1) * (D // n)], held.at[i], came.at[i]) for i in range(n)]
        away = [pltpu.make_async_copy(held.at[i], dst.at[:, i * (D // n) : (i + 1) * (D // n)], went.at[i]) for i in range(n)]
        for copy in into:
            copy.start()
        for i in range(n):
            into[i].wait()
            away[i].start()
        for copy in away:
            copy.wait()

    return pl.pallas_call(
        move,
        in_specs=[anywhere],
        out_specs=anywhere,
        out_shape=jax.ShapeDtypeStruct((R, D), bf),
        scratch_shapes=[V((n, R, D // n), bf), DMA((n,)), DMA((n,))],
        compiler_params=pltpu.CompilerParams(vmem_limit_bytes=64_000_000),
    )(out[0])


def solution(mesh):
    tokens, columns = P(("dp", "tp"), None), P(None, "tp")
    return jax.shard_map(layer, mesh=mesh, in_specs=(tokens, P(None), columns, columns, columns, P("tp", None)), out_specs=tokens, check_vma=False)
```
